32 devices in a mesh: dp: 2 (over core), expert: 16 (over z, y, x).
Axes of the slice: x: 2, y: 2, z: 4, core: 2. Of those that a mesh axis runs over, the one named last changes fastest.
Arguments:
- tokens: bfloat16 [2048, 4096], P(('dp', 'expert')), parts along dimension 0, may hold values from -6 to 6
- expert_ids: int32 [2048, 2], P(('dp', 'expert')), parts along dimension 0, may hold values from 0 to 7, all different within a row; in each aligned block of 64 rows (0 to 63, 64 to 127, ...) at most 24 rows name the same one
- route_weights: float32 [2048, 2], P(('dp', 'expert')), parts along dimension 0, may hold values from 0.1 to 1
- norm_gain: float32 [4096], replicated, may hold values from 0.1 to 1.9
- w_gate: bfloat16 [16, 4096, 896], P('expert'), may hold values from -0.09375 to 0.09375
- w_up: bfloat16 [16, 4096, 896], P('expert'), may hold values from -0.09375 to 0.09375
- w_down: bfloat16 [16, 896, 4096], P('expert'), may hold values from -0.125 to 0.125
Outputs:
- layer_out: bfloat16 [2048, 4096], P(('dp', 'expert')), parts along dimension 0
The draws below stay inside these ranges and needn't reach their ends.
There are 2 independent parts, one for each index of `dp`. The reference program is written for one: setup_inputs(seed, part) draws one part's arguments, and reference() takes and returns one part's arrays. A program takes and returns all parts, laid end to end along the dimension named above; an argument that names none is the same for every part. Nothing has to cross between parts.
Inputs may be any that keep to these rules, and one draw needn't show every extreme that they name: `expert_ids`: each token names two different experts; among the 64 tokens of one device no expert is named more than 24 times, a bound that some block reaches.
All inputs are finite; a program needn't handle non-finite values.
Results may differ from the reference program's by a relative error of at most 0.006.
Values may be sent and summed in bfloat16 or wider, within the bound.
No kernel may reach another device: no remote copies, remote signals or barrier semaphores. Data moves between devices by JAX's collectives and lax.ppermute only.
A program may use at most 128 MiB of HBM per device.

```python
import math
import jax
import jax.numpy as jnp
import numpy as np
from jax import lax

D = 4096
EXPERTS = 8
FF_DEV = 896
TOK_DEV = 64
FF = 1792
CAP = 24
TOKENS = 1024
N_EXPERT = 16


def level_of(key, shape, cuts, smallest, largest):
    def one(dim, parts):
        heights = jax.random.uniform(jax.random.fold_in(jax.random.fold_in(key, 6), dim), (parts,), jnp.float32, smallest / len(cuts), largest / len(cuts))
        return jnp.repeat(jnp.exp(heights), shape[dim] // parts).reshape((-1,) + (1,) * (len(shape) - dim - 1))

    loudness = one(*cuts[0])
    for cut in cuts[1:]:
        loudness = loudness * one(*cut)
    return loudness


def assign_block(key, own, number, rows, count, top, reach, skew):
    ranking = jax.random.permutation(key, count)
    packed, ordinary = portions_of(count, rows * top, reach, skew, True), portions_of(count, rows * top, reach, skew, False)
    places = jnp.arange(count)

    def named(sizes, rotation):
        used = int((sizes > 0).sum())
        fixed = max(1, used // 4)
        passed = fixed + (places - fixed + rotation * (used - fixed)) % max(1, count - fixed)
        return jnp.zeros((count,), jnp.int32).at[ranking[jnp.where(places < fixed, places, passed)]].set(jnp.asarray(sizes, jnp.int32))

    sizes = jnp.where(number % 4 == 0, named(packed, number // 4), named(ordinary, number - number // 4 - 1))
    mixed = jax.random.permutation(jax.random.fold_in(own, 3), count)
    giver, sink = mixed[0:count // 2 * 2:2], mixed[1:count // 2 * 2:2]
    margin = jnp.minimum(sizes[giver] - 1, reach - sizes[sink]) // 2
    margin = jnp.where((giver == ranking[0]) | (sink == ranking[0]) | (sizes[sink] == 0), 0, jnp.maximum(margin, 0))
    passed = jax.random.randint(jax.random.fold_in(own, 4), (count // 2,), 0, 1 << 20) % (margin + 1)
    sizes = sizes.at[giver].add(-passed).at[sink].add(passed)
    items = jnp.searchsorted(jnp.cumsum(sizes), jnp.arange(rows * top), side="right").astype(jnp.int32)
    grid = items.reshape(top, rows).T
    grid = grid[jax.random.permutation(jax.random.fold_in(own, 1), rows)]
    rotation = jax.random.randint(jax.random.fold_in(own, 2), (rows, 1), 0, top)
    return jnp.take_along_axis(grid, (jnp.arange(top)[None, :] + rotation) % top, axis=1)


def portions_of(amount, total, limit, skew, full):
    weights = [(1 << 20) // math.isqrt(standing ** skew) + 1 for standing in range(1, amount + 1)]
    largest = limit if full else min(limit, max(-(-total // amount), total * weights[0] // sum(weights)))
    least = 1 if total - largest >= amount - 1 else 0
    given, rest = [largest] + [least] * (amount - 1), total - largest - least * (amount - 1)
    while rest > 0:
        free = [i for i in range(1, amount) if given[i] < largest] or [i for i in range(1, amount) if given[i] < limit]
        whole, remaining = sum([weights[i] for i in free]), rest
        for i in free:
            addition = min(limit - given[i], max(1, remaining * weights[i] // whole), rest)
            given[i] = given[i] + addition
            rest = rest - addition
    return np.array(given)


def noise(rng, shape, deviation, limit, cuts=(), kind=jnp.bfloat16):
    entries = deviation * jax.random.normal(rng, shape, jnp.float32)
    if cuts:
        entries = entries * level_of(rng, shape, cuts, -0.22, 0.18)
    return jnp.clip(entries, -limit, limit).astype(kind)


def setup_inputs(seed: int = 0, part: int = 0) -> dict:
    streams_of = jax.random.split(jax.random.key(seed), 8)
    part_splits = jax.random.split(jax.random.fold_in(streams_of[7], part), 8)
    tokens = noise(part_splits[0], (TOKENS, D), 1.0, 6.0, ((0, 16),))
    expert_ids_keys = jax.random.split(jax.random.fold_in(part_splits[1], 1), TOKENS // TOK_DEV)
    expert_ids_turns = jax.random.permutation(jax.random.fold_in(part_splits[1], 3), TOKENS // TOK_DEV)
    expert_ids = jax.vmap(lambda own, number: assign_block(jax.random.fold_in(part_splits[1], 2), own, number, TOK_DEV, EXPERTS, 2, CAP, 2))(expert_ids_keys, expert_ids_turns).reshape((TOKENS, 2))
    route_weights = jnp.clip(0.1 + 0.9 * jax.random.uniform(part_splits[2], (TOKENS, 2), jnp.float32) ** level_of(part_splits[2], (TOKENS, 2), ((0, 16),), -0.2, 0.2), 0.1, 1.0)
    norm_gain = jnp.clip(1.0 + 0.18 * jax.random.normal(streams_of[3], (D,), jnp.float32), 0.1, 1.9)
    w_gate = noise(streams_of[4], (N_EXPERT, D, FF_DEV), D ** -0.5, 0.09375, ((0, 16),))
    w_up = noise(streams_of[5], (N_EXPERT, D, FF_DEV), D ** -0.5, 0.09375, ((0, 16),))
    w_down = noise(streams_of[6], (N_EXPERT, FF_DEV, D), FF ** -0.5, 0.125, ((0, 16),))
    return {"tokens": tokens, "expert_ids": expert_ids, "route_weights": route_weights, "norm_gain": norm_gain, "w_gate": w_gate, "w_up": w_up, "w_down": w_down}


def rms_norm(values, norm_gain):
    wide = values.astype(jnp.float32)
    mean_square = lax.optimization_barrier(jnp.mean(wide * wide, axis=-1, keepdims=True))
    return (wide * lax.rsqrt(mean_square + 1e-05) * norm_gain).astype(jnp.bfloat16)

def reference(tokens, expert_ids, route_weights, norm_gain, w_gate, w_up, w_down):
    shards = N_EXPERT // EXPERTS
    normed = rms_norm(tokens, norm_gain)
    flat_ids = expert_ids.reshape(N_EXPERT, TOK_DEV * 2)
    onehot = (flat_ids[:, :, None] == jnp.arange(EXPERTS, dtype=jnp.int32)[None, None, :]).astype(jnp.int32)
    rank_in = lax.optimization_barrier(jnp.sum((jnp.cumsum(onehot, axis=1) - onehot) * onehot, axis=-1)).astype(jnp.int32)
    source = jnp.broadcast_to(jnp.arange(N_EXPERT, dtype=jnp.int32)[:, None], flat_ids.shape)
    tok_index = source * TOK_DEV + (jnp.arange(TOK_DEV * 2, dtype=jnp.int32) // 2)[None, :]
    slots = jnp.zeros((EXPERTS, N_EXPERT, CAP, D), jnp.bfloat16)
    slots = slots.at[flat_ids, source, rank_in].set(normed[tok_index])

    def one_expert(expert):
        row_block = slots[expert].reshape(N_EXPERT * CAP, D)
        start = (expert * shards).astype(jnp.int32)
        gate_full = lax.dynamic_slice_in_dim(w_gate, start, shards, 0).transpose(1, 0, 2).reshape(D, shards * FF_DEV)
        up_full = lax.dynamic_slice_in_dim(w_up, start, shards, 0).transpose(1, 0, 2).reshape(D, shards * FF_DEV)
        down_full = lax.dynamic_slice_in_dim(w_down, start, shards, 0).reshape(shards * FF_DEV, D)
        gate_act = jnp.dot(row_block, gate_full, preferred_element_type=jnp.float32)
        up_act = jnp.dot(row_block, up_full, preferred_element_type=jnp.float32)
        hidden = (jax.nn.silu(gate_act) * up_act).astype(jnp.bfloat16)
        expert_out = jnp.dot(hidden, down_full, preferred_element_type=jnp.float32)
        return expert_out.reshape(N_EXPERT, CAP, D)
    outputs = lax.map(one_expert, jnp.arange(EXPERTS, dtype=jnp.int32))
    picked = outputs[flat_ids, source, rank_in].reshape(TOKENS, 2, D)
    mixture = lax.optimization_barrier(jnp.sum(route_weights[:, :, None] * picked, axis=1))
    return (tokens.astype(jnp.float32) + mixture).astype(jnp.bfloat16)
```

```python
import jax
import jax.numpy as jnp
from jax import lax
from jax.sharding import PartitionSpec as P

EXPERTS = 8
CAP = 24
CHUNKS = 4


def rms_norm(values, norm_gain):
    wide = values.astype(jnp.float32)
    mean_square = jnp.mean(wide * wide, axis=-1, keepdims=True)
    return (wide * lax.rsqrt(mean_square + 1e-05) * norm_gain).astype(jnp.bfloat16)


def flip(values, mask, n_devices):
    if mask == 0:
        return values
    return lax.ppermute(values, "expert", [(i, i ^ mask) for i in range(n_devices)])


def body(tokens, expert_ids, route_weights, norm_gain, w_gate, w_up, w_down):
    n_devices = lax.axis_size("expert")
    shards = n_devices // EXPERTS
    tok_count, width = tokens.shape
    own_expert = lax.axis_index("expert") // shards
    normed = rms_norm(tokens, norm_gain)

    flat_ids = jnp.bitwise_xor(expert_ids, own_expert).reshape(tok_count * 2)
    onehot = (flat_ids[:, None] == jnp.arange(EXPERTS, dtype=jnp.int32)[None, :]).astype(jnp.int32)
    rank_in = jnp.sum((jnp.cumsum(onehot, axis=0) - onehot) * onehot, axis=1)
    slot_index = (flat_ids * CAP + rank_in).reshape(tok_count, 2)
    columns = jnp.arange(EXPERTS * CAP, dtype=jnp.int32)
    hits = slot_index[:, :, None] == columns[None, None, :]
    selector = jnp.any(hits, axis=1).T.astype(jnp.bfloat16)
    slots = jnp.dot(selector, normed, preferred_element_type=jnp.float32).astype(jnp.bfloat16)
    slots = slots.reshape(EXPERTS, CAP, width)
    picker = hits.transpose(1, 0, 2).reshape(2 * tok_count, EXPERTS, CAP).astype(jnp.bfloat16)
    weights = route_weights.T.reshape(2 * tok_count, 1)

    per = EXPERTS // CHUNKS
    mine = []
    for c in range(CHUNKS):
        blocks = [flip(slots[r], r * shards, n_devices) for r in range(c * per, (c + 1) * per)]
        mine.append(jnp.concatenate(blocks, axis=0))
    rows = per * CAP
    total = tokens.astype(jnp.float32)
    for c in range(CHUNKS):
        group = [flip(mine[c], m, n_devices) for m in range(shards)]
        row_block = jnp.concatenate(group, axis=0)
        gate_act = jnp.dot(row_block, w_gate[0], preferred_element_type=jnp.float32)
        up_act = jnp.dot(row_block, w_up[0], preferred_element_type=jnp.float32)
        hidden = (jax.nn.silu(gate_act) * up_act).astype(jnp.bfloat16)
        part = jnp.dot(hidden, w_down[0], preferred_element_type=jnp.float32)
        part = part.reshape(shards, rows, width)
        summed = part[0]
        for m in range(1, shards):
            summed = summed + flip(part[m].astype(jnp.bfloat16), m, n_devices).astype(jnp.float32)
        done = summed.astype(jnp.bfloat16).reshape(per, CAP, width)
        back = [flip(done[k], (c * per + k) * shards, n_devices) for k in range(per)]
        back = jnp.concatenate(back, axis=0)
        chosen = picker[:, c * per:(c + 1) * per].reshape(2 * tok_count, rows)
        picked = jnp.dot(chosen, back, preferred_element_type=jnp.float32)
        picked = (picked * weights).reshape(2, tok_count, width)
        total = total + picked[0] + picked[1]
    return total.astype(jnp.bfloat16)


def solution(mesh):
    in_specs = (
        P(("dp", "expert"), None),
        P(("dp", "expert"), None),
        P(("dp", "expert"), None),
        P(),
        P("expert", None, None),
        P("expert", None, None),
        P("expert", None, None),
    )
    out_specs = P(("dp", "expert"), None)
    return jax.shard_map(body, mesh=mesh, in_specs=in_specs, out_specs=out_specs, check_vma=False)
```

```python
import jax
import jax.numpy as jnp
from jax import lax
from jax.experimental import pallas as pl
from jax.experimental.pallas import tpu as pltpu
from jax.sharding import PartitionSpec as P


EXPERTS = 8
CAP = 24
CHUNKS = ((0, 1), (2, 3), (4,), (5,), (6,), (7,))
PREP_FLOPS = 20_000_000_000
VMEM = pl.BlockSpec(memory_space=pltpu.VMEM)


def flip(values, mask, n_devices):
    if mask == 0:
        return values
    return lax.ppermute(values, "expert", [(i, i ^ mask) for i in range(n_devices)])


def expert_kernel(blocks, *refs):
    rows_in, (w_gate, w_up, w_down), (mine, other, rows, hidden) = refs[:blocks], refs[blocks:blocks + 3], refs[blocks + 3:]
    at = 0
    for ref in rows_in:
        rows[pl.ds(at, ref.shape[0]), :] = ref[...]
        at += ref.shape[0]
    own = mine.shape[0]
    small = rows.shape[0] <= 256
    step = 128

    def first(n, carry):
        part = pl.ds(pl.multiple_of(n * step, step), step)
        both = jnp.concatenate([w_gate[0, :, part], w_up[0, :, part]], axis=1)
        acts = jnp.dot(rows[...], both, preferred_element_type=jnp.float32)
        gate_act, up_act = acts[:, :step], acts[:, step:]
        hidden[:, part] = (gate_act / (1.0 + jnp.exp(-gate_act)) * up_act).astype(jnp.bfloat16)
        return carry

    lax.fori_loop(0, w_gate.shape[2] // step, first, 0, unroll=small)
    wide = 256

    def second(n, carry):
        part = pl.ds(pl.multiple_of(n * wide, wide), wide)
        out = jnp.dot(hidden[...], w_down[0, :, part], preferred_element_type=jnp.float32)
        mine[:, part] = out[:own]
        other[:, part] = out[own:].astype(jnp.bfloat16)
        return carry

    lax.fori_loop(0, w_down.shape[2] // wide, second, 0, unroll=small)


def prepare_kernel(own_expert, ids, weights, tokens, norm_gain, *outs):
    blocks, table = outs[:EXPERTS], outs[EXPERTS]
    count = tokens.shape[0]
    wide = tokens[...].astype(jnp.float32)
    mean_square = jnp.mean(wide * wide, axis=-1, keepdims=True)
    normed = (wide * lax.rsqrt(mean_square + 1e-05) * norm_gain[...]).astype(jnp.bfloat16)
    relative = jnp.bitwise_xor(ids[...], own_expert[0])
    expert = lax.broadcasted_iota(jnp.int32, (EXPERTS, count), 0)
    first, second = relative[0:1] == expert, relative[1:2] == expert
    named = jnp.where(first | second, 1.0, 0.0)
    earlier = lax.broadcasted_iota(jnp.int32, (count, count), 0) < lax.broadcasted_iota(jnp.int32, (count, count), 1)
    rank = jnp.dot(named, jnp.where(earlier, 1.0, 0.0), preferred_element_type=jnp.float32)
    place = jnp.where(first | second, rank.astype(jnp.int32), -1)
    share = jnp.where(first, weights[0:1], jnp.where(second, weights[1:2], 0.0))
    row = lax.broadcasted_iota(jnp.int32, (CAP, count), 0)
    for r in range(EXPERTS):
        hit = place[r:r + 1] == row
        pick = jnp.where(hit, 1.0, 0.0).astype(jnp.bfloat16)
        blocks[r][...] = jnp.dot(pick, normed, preferred_element_type=jnp.float32).astype(jnp.bfloat16)
        table[r * CAP:(r + 1) * CAP, :] = jnp.where(hit, share[r:r + 1], 0.0)


def prepare(own_expert, ids, weights, tokens, norm_gain):
    count, width = tokens.shape
    *blocks, table = pl.pallas_call(
        prepare_kernel,
        out_shape=[jax.ShapeDtypeStruct((CAP, width), jnp.bfloat16)] * EXPERTS
        + [jax.ShapeDtypeStruct((EXPERTS * CAP, count), jnp.float32)],
        in_specs=[pl.BlockSpec(memory_space=pltpu.SMEM)] + [VMEM] * 4,
        out_specs=[VMEM] * (EXPERTS + 1),
        cost_estimate=pl.CostEstimate(flops=PREP_FLOPS, bytes_accessed=4 * count * width, transcendentals=count),
        compiler_params=pltpu.CompilerParams(vmem_limit_bytes=8 << 20),
    )(own_expert, ids, weights, tokens, norm_gain)
    return blocks, table


def combine_kernel(tokens, table, *refs):
    blocks, out, rows = refs[:EXPERTS], refs[EXPERTS], refs[EXPERTS + 1]
    for r in range(EXPERTS):
        rows[pl.ds(r * CAP, CAP), :] = blocks[r][...]
    share = table[...].T
    high = share.astype(jnp.bfloat16)
    low = (share - high.astype(jnp.float32)).astype(jnp.bfloat16)
    mixture = jnp.dot(high, rows[...], preferred_element_type=jnp.float32)
    mixture = mixture + jnp.dot(low, rows[...], preferred_element_type=jnp.float32)
    out[...] = (tokens[...].astype(jnp.float32) + mixture).astype(jnp.bfloat16)


def combine(tokens, table, blocks):
    count, width = tokens.shape
    return pl.pallas_call(
        combine_kernel,
        out_shape=jax.ShapeDtypeStruct((count, width), jnp.bfloat16),
        in_specs=[VMEM] * (EXPERTS + 2),
        out_specs=VMEM,
        scratch_shapes=[pltpu.VMEM((EXPERTS * CAP, width), jnp.bfloat16)],
        cost_estimate=pl.CostEstimate(flops=4 * count * EXPERTS * CAP * width, bytes_accessed=4 * count * width, transcendentals=0),
        compiler_params=pltpu.CompilerParams(vmem_limit_bytes=12 << 20),
    )(tokens, table, *blocks)


def experts(own, others, w_gate, w_up, w_down):
    count = sum(b.shape[0] for b in own)
    total = count + sum(b.shape[0] for b in others)
    width, units = w_gate.shape[1:]
    blocks = len(own) + len(others)
    return pl.pallas_call(
        lambda *refs: expert_kernel(blocks, *refs),
        out_shape=(
            jax.ShapeDtypeStruct((count, width), jnp.float32),
            jax.ShapeDtypeStruct((total - count, width), jnp.bfloat16),
        ),
        in_specs=[VMEM] * (blocks + 3),
        out_specs=(VMEM, VMEM),
        scratch_shapes=[pltpu.VMEM((total, width), jnp.bfloat16), pltpu.VMEM((total, units), jnp.bfloat16)],
        cost_estimate=pl.CostEstimate(flops=6 * max(total, 192) * width * units, bytes_accessed=6 * width * units, transcendentals=total * units),
        compiler_params=pltpu.CompilerParams(vmem_limit_bytes=(6 << 20) + total * (width + units) * 2),
    )(*own, *others, w_gate, w_up, w_down)


def body(tokens, expert_ids, route_weights, norm_gain, w_gate, w_up, w_down):
    n_devices = lax.axis_size("expert")
    shards = n_devices // EXPERTS
    own_expert = (lax.axis_index("expert") // shards).reshape(1).astype(jnp.int32)
    slots, table = prepare(own_expert, expert_ids.T, route_weights.T, tokens, norm_gain[None, :])
    mine = [flip(slots[r], r * shards, n_devices) for r in range(EXPERTS)]
    theirs = [[flip(mine[r], m, n_devices) for r in range(EXPERTS)] for m in range(1, shards)]
    back = [None] * EXPERTS
    for rs in CHUNKS:
        own = [mine[r] for r in rs]
        others = [theirs[m][r] for m in range(shards - 1) for r in rs]
        summed, part = experts(own, others, w_gate, w_up, w_down)
        rows = len(rs) * CAP
        for m in range(1, shards):
            summed = summed + flip(part[(m - 1) * rows:m * rows], m, n_devices).astype(jnp.float32)
        for i, r in enumerate(rs):
            done = summed[i * CAP:(i + 1) * CAP].astype(jnp.bfloat16)
            back[r] = flip(done, r * shards, n_devices)
    return combine(tokens, table, back)


def solution(mesh):
    in_specs = (
        P(("dp", "expert"), None),
        P(("dp", "expert"), None),
        P(("dp", "expert"), None),
        P(),
        P("expert", None, None),
        P("expert", None, None),
        P("expert", None, None),
    )
    out_specs = P(("dp", "expert"), None)
    return jax.shard_map(body, mesh=mesh, in_specs=in_specs, out_specs=out_specs, check_vma=False)
```

```python
import jax
import jax.numpy as jnp
from jax import lax
from jax.experimental import pallas as pl
from jax.experimental.pallas import tpu as pltpu
from jax.sharding import PartitionSpec as P


EXPERTS = 8
CAP = 24
CHUNKS = ((0, 1), (2, 3), (4, 5), (6, 7))
PREP_FLOPS = 20_000_000_000
VMEM = pl.BlockSpec(memory_space=pltpu.VMEM)


def flip(values, mask, n_devices):
    if mask == 0:
        return values
    return lax.ppermute(values, "expert", [(i, i ^ mask) for i in range(n_devices)])


def expert_kernel(blocks, *refs):
    rows_in, (w_gate, w_up, w_down), (mine, other, rows, hidden) = refs[:blocks], refs[blocks:blocks + 3], refs[blocks + 3:]
    at = 0
    for ref in rows_in:
        rows[pl.ds(at, ref.shape[0]), :] = ref[...]
        at += ref.shape[0]
    own = mine.shape[0]
    small = rows.shape[0] <= 256
    step = 128

    def first(n, carry):
        part = pl.ds(pl.multiple_of(n * step, step), step)
        both = jnp.concatenate([w_gate[0, :, part], w_up[0, :, part]], axis=1)
        acts = jnp.dot(rows[...], both, preferred_element_type=jnp.float32)
        gate_act, up_act = acts[:, :step], acts[:, step:]
        hidden[:, part] = (gate_act / (1.0 + jnp.exp(-gate_act)) * up_act).astype(jnp.bfloat16)
        return carry

    lax.fori_loop(0, w_gate.shape[2] // step, first, 0, unroll=small)
    wide = 256

    def second(n, carry):
        part = pl.ds(pl.multiple_of(n * wide, wide), wide)
        out = jnp.dot(hidden[...], w_down[0, :, part], preferred_element_type=jnp.float32)
        mine[:, part] = out[:own]
        other[:, part] = out[own:].astype(jnp.bfloat16)
        return carry

    lax.fori_loop(0, w_down.shape[2] // wide, second, 0, unroll=small)


def prepare_kernel(own_expert, *refs):
    given, blocks, table = refs[:4], refs[4:4 + EXPERTS], refs[4 + EXPERTS]
    held, sems = refs[5 + EXPERTS:9 + EXPERTS], refs[9 + EXPERTS]
    ids, weights, tokens, norm_gain = held
    copies = [pltpu.make_async_copy(a, b, sems.at[i]) for i, (a, b) in enumerate(zip(given, held))]
    for copy in copies:
        copy.start()
    for copy in copies:
        copy.wait()
    count = tokens.shape[0]
    wide = tokens[...].astype(jnp.float32)
    mean_square = jnp.mean(wide * wide, axis=-1, keepdims=True)
    normed = (wide * lax.rsqrt(mean_square + 1e-05) * norm_gain[...]).astype(jnp.bfloat16)
    relative = jnp.bitwise_xor(ids[...], own_expert[0])
    expert = lax.broadcasted_iota(jnp.int32, (EXPERTS, count), 0)
    first, second = relative[0:1] == expert, relative[1:2] == expert
    named = jnp.where(first | second, 1.0, 0.0)
    earlier = lax.broadcasted_iota(jnp.int32, (count, count), 0) < lax.broadcasted_iota(jnp.int32, (count, count), 1)
    rank = jnp.dot(named, jnp.where(earlier, 1.0, 0.0), preferred_element_type=jnp.float32)
    place = jnp.where(first | second, rank.astype(jnp.int32), -1)
    share = jnp.where(first, weights[0:1], jnp.where(second, weights[1:2], 0.0))
    row = lax.broadcasted_iota(jnp.int32, (CAP, count), 0)
    for r in range(EXPERTS):
        hit = place[r:r + 1] == row
        pick = jnp.where(hit, 1.0, 0.0).astype(jnp.bfloat16)
        blocks[r][...] = jnp.dot(pick, normed, preferred_element_type=jnp.float32).astype(jnp.bfloat16)
        table[r * CAP:(r + 1) * CAP, :] = jnp.where(hit, share[r:r + 1], 0.0)


def prepare(own_expert, ids, weights, tokens, norm_gain):
    count, width = tokens.shape
    given = [pltpu.with_memory_space_constraint(a, pltpu.HBM) for a in (ids, weights, tokens, norm_gain)]
    *blocks, table = pl.pallas_call(
        prepare_kernel,
        out_shape=[jax.ShapeDtypeStruct((CAP, width), jnp.bfloat16)] * EXPERTS
        + [jax.ShapeDtypeStruct((EXPERTS * CAP, count), jnp.float32)],
        in_specs=[pl.BlockSpec(memory_space=pltpu.SMEM)] + [pl.BlockSpec(memory_space=pltpu.HBM)] * 4,
        out_specs=[VMEM] * (EXPERTS + 1),
        scratch_shapes=[pltpu.VMEM(a.shape, a.dtype) for a in given] + [pltpu.SemaphoreType.DMA((4,))],
        cost_estimate=pl.CostEstimate(flops=PREP_FLOPS, bytes_accessed=4 * count * width, transcendentals=count),
        compiler_params=pltpu.CompilerParams(vmem_limit_bytes=8 << 20),
    )(own_expert, *given)
    return blocks, table


def combine_kernel(tokens, table, *refs):
    blocks, out, rows = refs[:EXPERTS], refs[EXPERTS], refs[EXPERTS + 1]
    for r in range(EXPERTS):
        rows[pl.ds(r * CAP, CAP), :] = blocks[r][...]
    share = table[...].T
    high = share.astype(jnp.bfloat16)
    low = (share - high.astype(jnp.float32)).astype(jnp.bfloat16)
    mixture = jnp.dot(high, rows[...], preferred_element_type=jnp.float32)
    mixture = mixture + jnp.dot(low, rows[...], preferred_element_type=jnp.float32)
    out[...] = (tokens[...].astype(jnp.float32) + mixture).astype(jnp.bfloat16)


def combine(tokens, table, blocks):
    count, width = tokens.shape
    return pl.pallas_call(
        combine_kernel,
        out_shape=jax.ShapeDtypeStruct((count, width), jnp.bfloat16),
        in_specs=[VMEM] * (EXPERTS + 2),
        out_specs=VMEM,
        scratch_shapes=[pltpu.VMEM((EXPERTS * CAP, width), jnp.bfloat16)],
        cost_estimate=pl.CostEstimate(flops=4 * count * EXPERTS * CAP * width, bytes_accessed=4 * count * width, transcendentals=0),
        compiler_params=pltpu.CompilerParams(vmem_limit_bytes=12 << 20),
    )(tokens, table, *blocks)


def experts(own, others, w_gate, w_up, w_down):
    count = sum(b.shape[0] for b in own)
    total = count + sum(b.shape[0] for b in others)
    width, units = w_gate.shape[1:]
    blocks = len(own) + len(others)
    return pl.pallas_call(
        lambda *refs: expert_kernel(blocks, *refs),
        out_shape=(
            jax.ShapeDtypeStruct((count, width), jnp.float32),
            jax.ShapeDtypeStruct((total - count, width), jnp.bfloat16),
        ),
        in_specs=[VMEM] * (blocks + 3),
        out_specs=(VMEM, VMEM),
        scratch_shapes=[pltpu.VMEM((total, width), jnp.bfloat16), pltpu.VMEM((total, units), jnp.bfloat16)],
        cost_estimate=pl.CostEstimate(flops=6 * max(total, 192) * width * units, bytes_accessed=6 * width * units, transcendentals=total * units),
        compiler_params=pltpu.CompilerParams(vmem_limit_bytes=(6 << 20) + total * (width + units) * 2),
    )(*own, *others, w_gate, w_up, w_down)


def body(tokens, expert_ids, route_weights, norm_gain, w_gate, w_up, w_down):
    n_devices = lax.axis_size("expert")
    shards = n_devices // EXPERTS
    own_expert = (lax.axis_index("expert") // shards).reshape(1).astype(jnp.int32)
    slots, table = prepare(own_expert, expert_ids.T, route_weights.T, tokens, norm_gain[None, :])
    mine = [flip(slots[r], r * shards, n_devices) for r in range(EXPERTS)]
    theirs = [[flip(mine[r], m, n_devices) for r in range(EXPERTS)] for m in range(1, shards)]
    back = [None] * EXPERTS
    for rs in CHUNKS:
        own = [mine[r] for r in rs]
        others = [theirs[m][r] for m in range(shards - 1) for r in rs]
        summed, part = experts(own, others, w_gate, w_up, w_down)
        rows = len(rs) * CAP
        for m in range(1, shards):
            summed = summed + flip(part[(m - 1) * rows:m * rows], m, n_devices).astype(jnp.float32)
        for i, r in enumerate(rs):
            done = summed[i * CAP:(i + 1) * CAP].astype(jnp.bfloat16)
            back[r] = flip(done, r * shards, n_devices)
    return combine(tokens, table, back)


def solution(mesh):
    in_specs = (
        P(("dp", "expert"), None),
        P(("dp", "expert"), None),
        P(("dp", "expert"), None),
        P(),
        P("expert", None, None),
        P("expert", None, None),
        P("expert", None, None),
    )
    out_specs = P(("dp", "expert"), None)
    return jax.shard_map(body, mesh=mesh, in_specs=in_specs, out_specs=out_specs, check_vma=False)
```

```python
import jax
import jax.numpy as jnp
from jax import lax
from jax.experimental import pallas as pl
from jax.experimental.pallas import tpu as pltpu
from jax.sharding import PartitionSpec as P


EXPERTS = 8
CAP = 24
CHUNKS = ((0, 1), (2, 3), (4, 5), (6, 7))
PREP_FLOPS = 20_000_000_000
VMEM = pl.BlockSpec(memory_space=pltpu.VMEM)


def flip(values, mask, n_devices):
    if mask == 0:
        return values
    return lax.ppermute(values, "expert", [(i, i ^ mask) for i in range(n_devices)])


def expert_kernel(blocks, *refs):
    rows_in, (w_gate, w_up, w_down), (mine, other, rows, hidden) = refs[:blocks], refs[blocks:blocks + 3], refs[blocks + 3:]
    at = 0
    for ref in rows_in:
        rows[pl.ds(at, ref.shape[0]), :] = ref[...]
        at += ref.shape[0]
    own = mine.shape[0]
    small = rows.shape[0] <= 256
    step = 128

    def first(n, carry):
        part = pl.ds(pl.multiple_of(n * step, step), step)
        both = jnp.concatenate([w_gate[0, :, part], w_up[0, :, part]], axis=1)
        acts = jnp.dot(rows[...], both, preferred_element_type=jnp.float32)
        gate_act, up_act = acts[:, :step], acts[:, step:]
        hidden[:, part] = (gate_act / (1.0 + jnp.exp(-gate_act)) * up_act).astype(jnp.bfloat16)
        return carry

    lax.fori_loop(0, w_gate.shape[2] // step, first, 0, unroll=small)
    wide = 256

    def second(n, carry):
        part = pl.ds(pl.multiple_of(n * wide, wide), wide)
        out = jnp.dot(hidden[...], w_down[0, :, part], preferred_element_type=jnp.float32)
        mine[:, part] = out[:own]
        other[:, part] = out[own:].astype(jnp.bfloat16)
        return carry

    lax.fori_loop(0, w_down.shape[2] // wide, second, 0, unroll=small)


def prepare_kernel(own_expert, *refs):
    given, blocks, table = refs[:4], refs[4:4 + EXPERTS], refs[4 + EXPERTS]
    held, sems = refs[5 + EXPERTS:9 + EXPERTS], refs[9 + EXPERTS]
    ids, weights, tokens, norm_gain = held
    copies = [pltpu.make_async_copy(a, b, sems.at[i]) for i, (a, b) in enumerate(zip(given, held))]
    for copy in copies:
        copy.start()
    for copy in copies:
        copy.wait()
    count = tokens.shape[0]
    wide = tokens[...].astype(jnp.float32)
    mean_square = jnp.mean(wide * wide, axis=-1, keepdims=True)
    normed = (wide * lax.rsqrt(mean_square + 1e-05) * norm_gain[...]).astype(jnp.bfloat16)
    relative = jnp.bitwise_xor(ids[...], own_expert[0])
    expert = lax.broadcasted_iota(jnp.int32, (EXPERTS, count), 0)
    first, second = relative[0:1] == expert, relative[1:2] == expert
    named = jnp.where(first | second, 1.0, 0.0)
    earlier = lax.broadcasted_iota(jnp.int32, (count, count), 0) < lax.broadcasted_iota(jnp.int32, (count, count), 1)
    rank = jnp.dot(named, jnp.where(earlier, 1.0, 0.0), preferred_element_type=jnp.float32)
    place = jnp.where(first | second, rank.astype(jnp.int32), -1)
    share = jnp.where(first, weights[0:1], jnp.where(second, weights[1:2], 0.0))
    row = lax.broadcasted_iota(jnp.int32, (CAP, count), 0)
    for r in range(EXPERTS):
        hit = place[r:r + 1] == row
        pick = jnp.where(hit, 1.0, 0.0).astype(jnp.bfloat16)
        blocks[r][...] = jnp.dot(pick, normed, preferred_element_type=jnp.float32).astype(jnp.bfloat16)
        table[r * CAP:(r + 1) * CAP, :] = jnp.where(hit, share[r:r + 1], 0.0)


def prepare(own_expert, ids, weights, tokens, norm_gain):
    count, width = tokens.shape
    given = [pltpu.with_memory_space_constraint(a, pltpu.HBM) for a in (ids, weights, tokens, norm_gain)]
    *blocks, table = pl.pallas_call(
        prepare_kernel,
        out_shape=[jax.ShapeDtypeStruct((CAP, width), jnp.bfloat16)] * EXPERTS
        + [jax.ShapeDtypeStruct((EXPERTS * CAP, count), jnp.float32)],
        in_specs=[pl.BlockSpec(memory_space=pltpu.SMEM)] + [pl.BlockSpec(memory_space=pltpu.HBM)] * 4,
        out_specs=[VMEM] * (EXPERTS + 1),
        scratch_shapes=[pltpu.VMEM(a.shape, a.dtype) for a in given] + [pltpu.SemaphoreType.DMA((4,))],
        cost_estimate=pl.CostEstimate(flops=PREP_FLOPS, bytes_accessed=4 * count * width, transcendentals=count),
        compiler_params=pltpu.CompilerParams(vmem_limit_bytes=8 << 20),
    )(own_expert, *given)
    return blocks, table


def combine_kernel(picked, base, table, *refs):
    blocks, out, rows = refs[:-2], refs[-2], refs[-1]
    for i, ref in enumerate(blocks):
        rows[pl.ds(i * CAP, CAP), :] = ref[...]
    share = jnp.concatenate([table[r * CAP:(r + 1) * CAP, :] for r in picked], axis=0).T
    high = share.astype(jnp.bfloat16)
    low = (share - high.astype(jnp.float32)).astype(jnp.bfloat16)
    mixture = jnp.dot(high, rows[...], preferred_element_type=jnp.float32)
    mixture = mixture + jnp.dot(low, rows[...], preferred_element_type=jnp.float32)
    out[...] = (base[...].astype(jnp.float32) + mixture).astype(out.dtype)


def combine(base, table, blocks, picked, kind):
    count, width = base.shape
    return pl.pallas_call(
        lambda *refs: combine_kernel(picked, *refs),
        out_shape=jax.ShapeDtypeStruct((count, width), kind),
        in_specs=[VMEM] * (len(picked) + 2),
        out_specs=VMEM,
        scratch_shapes=[pltpu.VMEM((len(picked) * CAP, width), jnp.bfloat16)],
        cost_estimate=pl.CostEstimate(flops=4 * count * len(picked) * CAP * width, bytes_accessed=4 * count * width, transcendentals=0),
        compiler_params=pltpu.CompilerParams(vmem_limit_bytes=12 << 20),
    )(base, table, *[blocks[r] for r in picked])


def experts(own, others, w_gate, w_up, w_down):
    count = sum(b.shape[0] for b in own)
    total = count + sum(b.shape[0] for b in others)
    width, units = w_gate.shape[1:]
    blocks = len(own) + len(others)
    return pl.pallas_call(
        lambda *refs: expert_kernel(blocks, *refs),
        out_shape=(
            jax.ShapeDtypeStruct((count, width), jnp.float32),
            jax.ShapeDtypeStruct((total - count, width), jnp.bfloat16),
        ),
        in_specs=[VMEM] * (blocks + 3),
        out_specs=(VMEM, VMEM),
        scratch_shapes=[pltpu.VMEM((total, width), jnp.bfloat16), pltpu.VMEM((total, units), jnp.bfloat16)],
        cost_estimate=pl.CostEstimate(flops=6 * max(total, 192) * width * units, bytes_accessed=6 * width * units, transcendentals=total * units),
        compiler_params=pltpu.CompilerParams(vmem_limit_bytes=(6 << 20) + total * (width + units) * 2),
    )(*own, *others, w_gate, w_up, w_down)


def body(tokens, expert_ids, route_weights, norm_gain, w_gate, w_up, w_down):
    n_devices = lax.axis_size("expert")
    shards = n_devices // EXPERTS
    own_expert = (lax.axis_index("expert") // shards).reshape(1).astype(jnp.int32)
    slots, table = prepare(own_expert, expert_ids.T, route_weights.T, tokens, norm_gain[None, :])
    mine = [flip(slots[r], r * shards, n_devices) for r in range(EXPERTS)]
    theirs = [[flip(mine[r], m, n_devices) for r in range(EXPERTS)] for m in range(1, shards)]
    back = [None] * EXPERTS
    for rs in CHUNKS:
        own = [mine[r] for r in rs]
        others = [theirs[m][r] for m in range(shards - 1) for r in rs]
        summed, part = experts(own, others, w_gate, w_up, w_down)
        rows = len(rs) * CAP
        for m in range(1, shards):
            summed = summed + flip(part[(m - 1) * rows:m * rows], m, n_devices).astype(jnp.float32)
        for i, r in enumerate(rs):
            done = summed[i * CAP:(i + 1) * CAP].astype(jnp.bfloat16)
            back[r] = flip(done, r * shards, n_devices)
    early = combine(tokens, table, back, (2, 3, 4, 5), jnp.float32)
    return combine(early, table, back, (6, 7, 0, 1), tokens.dtype)


def solution(mesh):
    in_specs = (
        P(("dp", "expert"), None),
        P(("dp", "expert"), None),
        P(("dp", "expert"), None),
        P(),
        P("expert", None, None),
        P("expert", None, None),
        P("expert", None, None),
    )
    out_specs = P(("dp", "expert"), None)
    return jax.shard_map(body, mesh=mesh, in_specs=in_specs, out_specs=out_specs, check_vma=False)
```
